32 devices in a mesh: seq: 4 (over y, x), fsdp: 8 (over z, core).
Axes of the slice: x: 2, y: 2, z: 4, core: 2. Of those that a mesh axis runs over, the one named last changes fastest.
Arguments:
- audio_codes: int32 [8, 4, 1536], P('fsdp'), may hold values from 0 to 2047
- delay_masks: int32 [8, 4, 1536], P('fsdp'), may hold values from 0 to 1, as said below
- clip_lengths: int32 [8], P('fsdp'), may hold values from 768 to 1536, as said below
- text_states: bfloat16 [8, 64, 1024], P('fsdp'), may hold values from -6 to 6
- step_count: int32 [1], replicated, may hold values from 1 to 20
- attention_master: float32 [1, 8, 1024, 1024], P(None, None, ('seq', 'fsdp')), as said below
- attention_mean: float32 [1, 8, 1024, 1024], P(None, None, ('seq', 'fsdp')), may hold values from -5.722046e-06 to 5.722046e-06
- attention_square: float32 [1, 8, 1024, 1024], P(None, None, ('seq', 'fsdp')), may hold values from 8.6677144e-13 to 1.4446191e-11
- feedforward_master: float32 [1, 2, 1024, 4096], P(None, None, ('seq', 'fsdp')), may hold values from -0.1875 to 0.1875
- feedforward_mean: float32 [1, 2, 1024, 4096], P(None, None, ('seq', 'fsdp')), may hold values from -5.722046e-06 to 5.722046e-06
- feedforward_square: float32 [1, 2, 1024, 4096], P(None, None, ('seq', 'fsdp')), may hold values from 8.6677144e-13 to 1.4446191e-11
- tables_master: float32 [2, 4, 2048, 1024], P(None, None, ('seq', 'fsdp')), may hold values from -1 to 1, as said below
- tables_mean: float32 [2, 4, 2048, 1024], P(None, None, ('seq', 'fsdp')), may hold values from -5.722046e-06 to 5.722046e-06
- tables_square: float32 [2, 4, 2048, 1024], P(None, None, ('seq', 'fsdp')), may hold values from 8.6677144e-13 to 1.4446191e-11
- ahead_master: float32 [1024, 1024], P(('seq', 'fsdp')), may hold values from -0.1875 to 0.1875
- ahead_mean: float32 [1024, 1024], P(('seq', 'fsdp')), may hold values from -5.722046e-06 to 5.722046e-06
- ahead_square: float32 [1024, 1024], P(('seq', 'fsdp')), may hold values from 8.6677144e-13 to 1.4446191e-11
- norms_master: float32 [4, 2, 1024], P(None, None, ('seq', 'fsdp')), may hold values from -1 to 2, as said below
- norms_mean: float32 [4, 2, 1024], P(None, None, ('seq', 'fsdp')), may hold values from -5.722046e-06 to 5.722046e-06
- norms_square: float32 [4, 2, 1024], P(None, None, ('seq', 'fsdp')), may hold values from 8.6677144e-13 to 1.4446191e-11
Outputs:
- loss_value: float32 [], replicated
- gradient_norm: float32 [], replicated
- attention_master_new: float32 [1, 8, 1024, 1024], P(None, None, ('seq', 'fsdp'))
- attention_mean_new: float32 [1, 8, 1024, 1024], P(None, None, ('seq', 'fsdp'))
- attention_square_new: float32 [1, 8, 1024, 1024], P(None, None, ('seq', 'fsdp'))
- attention_rounded: bfloat16 [1, 8, 1024, 1024], P(None, None, ('seq', 'fsdp'))
- feedforward_master_new: float32 [1, 2, 1024, 4096], P(None, None, ('seq', 'fsdp'))
- feedforward_mean_new: float32 [1, 2, 1024, 4096], P(None, None, ('seq', 'fsdp'))
- feedforward_square_new: float32 [1, 2, 1024, 4096], P(None, None, ('seq', 'fsdp'))
- feedforward_rounded: bfloat16 [1, 2, 1024, 4096], P(None, None, ('seq', 'fsdp'))
- tables_master_new: float32 [2, 4, 2048, 1024], P(None, None, ('seq', 'fsdp'))
- tables_mean_new: float32 [2, 4, 2048, 1024], P(None, None, ('seq', 'fsdp'))
- tables_square_new: float32 [2, 4, 2048, 1024], P(None, None, ('seq', 'fsdp'))
- tables_rounded: bfloat16 [2, 4, 2048, 1024], P(None, None, ('seq', 'fsdp'))
- ahead_master_new: float32 [1024, 1024], P(('seq', 'fsdp'))
- ahead_mean_new: float32 [1024, 1024], P(('seq', 'fsdp'))
- ahead_square_new: float32 [1024, 1024], P(('seq', 'fsdp'))
- ahead_rounded: bfloat16 [1024, 1024], P(('seq', 'fsdp'))
- norms_master_new: float32 [4, 2, 1024], P(None, None, ('seq', 'fsdp'))
- norms_mean_new: float32 [4, 2, 1024], P(None, None, ('seq', 'fsdp'))
- norms_square_new: float32 [4, 2, 1024], P(None, None, ('seq', 'fsdp'))
- norms_rounded: bfloat16 [4, 2, 1024], P(None, None, ('seq', 'fsdp'))
The draws below stay inside these ranges and needn't reach their ends.
Inputs may be any that keep to these rules, and one draw needn't show every extreme that they name: `delay_masks`: 1 where codebook k's id at a frame counts as a target; always 0 at frames before frame k of the delay pattern. `clip_lengths`: targets at frames at or beyond a clip's length don't count; the first clip is full. `attention_master`: normal entries, scaled per matrix. `norms_master`: gains between 0.6 and 1.4, biases between -0.4 and 0.4. `tables_master`: entries of deviation about 1/16.
All inputs are finite; a program needn't handle non-finite values.
Results may differ from the reference program's by a relative error of at most 0.0055.
The reference program's roundings to bfloat16 on the way count: a program that leaves them out, or rounds other values in their place, can miss the bound.
Values may be sent and summed in bfloat16 or wider, within the bound.
A program may use at most 320 MiB of HBM per device.

```python
import math
import jax
import jax.numpy as jnp
from jax import lax

D = 1024
HEADS = 16
HD = 64
FF = 4096
CODEBOOKS = 4
VOCAB = 2048
NTXT = 64
LAYERS = 1
LEN = 1536
CLIPS = 8
NORMS = 4


def draw_clip_lengths(key, part):
    drawn_lengths = jax.random.randint(key, (CLIPS,), LEN // 2, LEN + 1)
    return drawn_lengths.at[0].set(LEN).astype(jnp.int32)


def draw_delay_masks(key, part):
    keep_draw = jax.random.randint(key, (CLIPS, CODEBOOKS, LEN), 0, 8) < 7
    frame_index = jnp.arange(LEN, dtype=jnp.int32)[None, None, :]
    codebook_index = jnp.arange(CODEBOOKS, dtype=jnp.int32)[None, :, None]
    return (keep_draw & (frame_index >= codebook_index)).astype(jnp.int32)


def draw_attention_master(key, part):
    base_draw = jax.random.truncated_normal(key, -4.0, 4.0, (LAYERS, 8, D, D), jnp.float32)
    factors = jnp.array([1.2, 1.2, 1.0, 4.0, 1.2, 1.2, 1.0, 4.0], jnp.float32) / math.sqrt(D)
    return base_draw * factors[None, :, None, None]


def norm_draws(key):
    gain_key = jax.random.fold_in(key, 11)
    bias_key = jax.random.fold_in(key, 12)
    gains = jax.random.uniform(gain_key, (3 * LAYERS + 1, 1, D), jnp.float32, 0.6, 1.4)
    biases = jax.random.uniform(bias_key, (3 * LAYERS + 1, 1, D), jnp.float32, -0.4, 0.4)
    return (gains, biases)


def draw_norms_master(key, part):
    gains, biases = norm_draws(key)
    return jnp.concatenate([gains, biases], axis=1)


def draw_tables_master(key, part):
    gains, biases = norm_draws(key)
    table_key = jax.random.fold_in(key, 21)
    base_draw = jax.random.truncated_normal(table_key, -4.0, 4.0, (2, CODEBOOKS, VOCAB, D), jnp.float32) * 0.0625
    shared = biases[3 * LAYERS, 0] * (20.0 / D)
    which = jnp.array([0.0, 1.0], jnp.float32)[:, None, None, None]
    return base_draw + which * shared[None, None, None, :]


def touch_ends(result, stream_key, least, top_value):
    longest = result.shape.index(max(result.shape))
    spots = []
    for shift in (0, 1):
        where = [jax.random.randint(jax.random.fold_in(stream_key, axis), (), 0, length) for axis, length in enumerate(result.shape)]
        where[longest] = (where[longest] + shift) % result.shape[longest]
        spots.append(tuple(where))
    return result.at[spots[0]].set(least).at[spots[1]].set(top_value)


def block_levels(stream_key, extent, cuts, low, top_value):
    def one(position, blocks):
        heights = jax.random.uniform(jax.random.fold_in(jax.random.fold_in(stream_key, 6), position), (blocks,), jnp.float32, low / len(cuts), top_value / len(cuts))
        return jnp.repeat(jnp.exp(heights), extent[position] // blocks).reshape((-1,) + (1,) * (len(extent) - position - 1))

    loudness = one(*cuts[0])
    for cut in cuts[1:]:
        loudness = loudness * one(*cut)
    return loudness


def gaussian(key, dims, spread, limit, shards=(), kind=jnp.bfloat16):
    drawn = jax.random.normal(key, dims, jnp.float32) * spread
    if len(shards) > 0:
        drawn = block_levels(key, dims, shards, -0.22, 0.18) * drawn
    return jnp.clip(drawn, min=-limit, max=limit).astype(kind)


def setup_inputs(seed: int = 0) -> dict:
    streams_of = jax.random.split(jax.random.key(seed), 21)
    return {
        "audio_codes": touch_ends(jax.random.randint(streams_of[0], (CLIPS, CODEBOOKS, LEN), 0, VOCAB), jax.random.fold_in(streams_of[0], 1), 0, VOCAB - 1).astype(jnp.int32),
        "delay_masks": draw_delay_masks(jax.random.fold_in(streams_of[20], 71), 0),
        "clip_lengths": draw_clip_lengths(jax.random.fold_in(streams_of[20], 71), 0),
        "text_states": gaussian(streams_of[3], (CLIPS, NTXT, D), 1.0, 6.0, ((0, 8),)),
        "step_count": jax.random.randint(streams_of[4], (1,), 1, 21).astype(jnp.int32),
        "attention_master": draw_attention_master(jax.random.fold_in(streams_of[20], 71), 0),
        "attention_mean": gaussian(streams_of[6], (LAYERS, 8, D, D), (0.0056 / (LAYERS * (8 * D * D + 2 * D * FF) + 2 * CODEBOOKS * VOCAB * D + D * D + 2 * NORMS * D) ** 0.5), 5.7220458984375e-06, ((2, 32),), jnp.float32),
        "attention_square": jnp.clip(jnp.exp(math.log(1.444619077139997e-11) - 2.8134107 * jax.random.uniform(streams_of[7], (LAYERS, 8, D, D), jnp.float32) ** block_levels(streams_of[7], (LAYERS, 8, D, D), ((2, 32),), -0.2, 0.2)), 8.667714441155938e-13, 1.444619077139997e-11),
        "feedforward_master": gaussian(streams_of[8], (LAYERS, 2, D, FF), D ** -0.5, 0.1875, ((2, 32),), jnp.float32),
        "feedforward_mean": gaussian(streams_of[9], (LAYERS, 2, D, FF), (0.0056 / (LAYERS * (8 * D * D + 2 * D * FF) + 2 * CODEBOOKS * VOCAB * D + D * D + 2 * NORMS * D) ** 0.5), 5.7220458984375e-06, ((2, 32),), jnp.float32),
        "feedforward_square": jnp.clip(jnp.exp(math.log(1.444619077139997e-11) - 2.8134107 * jax.random.uniform(streams_of[10], (LAYERS, 2, D, FF), jnp.float32) ** block_levels(streams_of[10], (LAYERS, 2, D, FF), ((2, 32),), -0.2, 0.2)), 8.667714441155938e-13, 1.444619077139997e-11),
        "tables_master": draw_tables_master(jax.random.fold_in(streams_of[20], 71), 0),
        "tables_mean": gaussian(streams_of[12], (2, CODEBOOKS, VOCAB, D), (0.0056 / (LAYERS * (8 * D * D + 2 * D * FF) + 2 * CODEBOOKS * VOCAB * D + D * D + 2 * NORMS * D) ** 0.5), 5.7220458984375e-06, ((2, 32),), jnp.float32),
        "tables_square": jnp.clip(jnp.exp(math.log(1.444619077139997e-11) - 2.8134107 * jax.random.uniform(streams_of[13], (2, CODEBOOKS, VOCAB, D), jnp.float32) ** block_levels(streams_of[13], (2, CODEBOOKS, VOCAB, D), ((2, 32),), -0.2, 0.2)), 8.667714441155938e-13, 1.444619077139997e-11),
        "ahead_master": gaussian(streams_of[14], (D, D), D ** -0.5, 0.1875, ((0, 32),), jnp.float32),
        "ahead_mean": gaussian(streams_of[15], (D, D), (0.0056 / (LAYERS * (8 * D * D + 2 * D * FF) + 2 * CODEBOOKS * VOCAB * D + D * D + 2 * NORMS * D) ** 0.5), 5.7220458984375e-06, ((0, 32),), jnp.float32),
        "ahead_square": jnp.clip(jnp.exp(math.log(1.444619077139997e-11) - 2.8134107 * jax.random.uniform(streams_of[16], (D, D), jnp.float32) ** block_levels(streams_of[16], (D, D), ((0, 32),), -0.2, 0.2)), 8.667714441155938e-13, 1.444619077139997e-11),
        "norms_master": draw_norms_master(jax.random.fold_in(streams_of[20], 71), 0),
        "norms_mean": gaussian(streams_of[18], (NORMS, 2, D), (0.0056 / (LAYERS * (8 * D * D + 2 * D * FF) + 2 * CODEBOOKS * VOCAB * D + D * D + 2 * NORMS * D) ** 0.5), 5.7220458984375e-06, ((2, 32),), jnp.float32),
        "norms_square": jnp.clip(jnp.exp(math.log(1.444619077139997e-11) - 2.8134107 * jax.random.uniform(streams_of[19], (NORMS, 2, D), jnp.float32) ** block_levels(streams_of[19], (NORMS, 2, D), ((2, 32),), -0.2, 0.2)), 8.667714441155938e-13, 1.444619077139997e-11),
    }


norm_epsilon = 1e-05
first_decay = 0.9
second_decay = 0.95
learn_rate = 0.03
weight_decay = 0.1
adam_epsilon = 1e-08
clip_limit = 0.05
ahead_weight = 0.3
masked_score = -1e+30

@jax.custom_vjp
def low(v):
    return lax.optimization_barrier(v.astype(jnp.bfloat16)).astype(jnp.float32)

@jax.custom_vjp
def low_back(v):
    return v

def low_keep(v):
    return (low(v), None)

def low_pass(kept, grad):
    return (grad,)

def back_keep(v):
    return (v, None)

def back_low(kept, grad):
    return (low(grad),)
low.defvjp(low_keep, low_pass)
low_back.defvjp(back_keep, back_low)

def highest_dot(left, right):
    return jnp.dot(left, right, precision=lax.Precision.HIGHEST, preferred_element_type=jnp.float32)

def layer_norm(residual, gain, bias):
    centered = residual - lax.optimization_barrier(jnp.mean(residual, axis=-1, keepdims=True))
    variance = lax.optimization_barrier(jnp.mean(centered * centered, axis=-1, keepdims=True))
    return centered * lax.rsqrt(variance + norm_epsilon) * gain + bias

def sinusoids(offset, row_count, width):
    half_width = width // 2
    log_rate = math.log(10000.0) / (half_width - 1)
    frequency = jnp.exp(jnp.arange(half_width, dtype=jnp.float32) * -log_rate)
    places = (offset + jnp.arange(row_count, dtype=jnp.float32))[:, None] * frequency[None, :]
    return jnp.concatenate([jnp.cos(places), jnp.sin(places)], axis=1)

def attend(queries, key_rows, value_rows, causal):
    row_count = queries.shape[0]
    query_heads = queries.reshape(row_count, HEADS, HD)
    key_heads = key_rows.reshape(key_rows.shape[0], HEADS, HD)
    value_heads = value_rows.reshape(value_rows.shape[0], HEADS, HD)
    scores = jnp.einsum('qhd,khd->hqk', query_heads, key_heads, precision=lax.Precision.HIGHEST) * (1.0 / math.sqrt(HD))
    scores = low_back(scores)
    if causal:
        allowed = jnp.arange(row_count)[:, None] >= jnp.arange(row_count)[None, :]
        scores = jnp.where(allowed[None], scores, masked_score)
    row_max = lax.optimization_barrier(jnp.max(scores, axis=2, keepdims=True))
    exponent = jnp.exp(scores - row_max)
    attention_probs = low(exponent / lax.optimization_barrier(jnp.sum(exponent, axis=2, keepdims=True)))
    mixture = jnp.einsum('hqk,khd->qhd', attention_probs, value_heads, precision=lax.Precision.HIGHEST)
    return low_back(low(mixture.reshape(row_count, D)))

def clip_loss(weights, codes_clip, masks_clip, length_clip, text_clip, position_table):
    attention_w, feedforward_w, tables_w, ahead_w, norms_w = weights
    residual = position_table
    for codebook in range(CODEBOOKS):
        residual = residual + jnp.take(tables_w[0, codebook], codes_clip[codebook], axis=0)
    residual = low_back(residual)
    for layer_index in range(LAYERS):
        matrices = attention_w[layer_index]
        base = 3 * layer_index
        normed = low(layer_norm(residual, norms_w[base, 0], norms_w[base, 1]))
        queries = low_back(low(highest_dot(normed, matrices[0])))
        key_rows = low_back(low(highest_dot(normed, matrices[1])))
        value_rows = low_back(low(highest_dot(normed, matrices[2])))
        residual = residual + low_back(highest_dot(attend(queries, key_rows, value_rows, True), matrices[3]))
        normed = low(layer_norm(residual, norms_w[base + 1, 0], norms_w[base + 1, 1]))
        cross_queries = low_back(low(highest_dot(normed, matrices[4])))
        cross_keys = low_back(low(highest_dot(text_clip, matrices[5])))
        cross_values = low_back(low(highest_dot(text_clip, matrices[6])))
        residual = residual + low_back(highest_dot(attend(cross_queries, cross_keys, cross_values, False), matrices[7]))
        normed = low(layer_norm(residual, norms_w[base + 2, 0], norms_w[base + 2, 1]))
        hidden = low_back(highest_dot(normed, feedforward_w[layer_index, 0]))
        hidden = low(jax.nn.gelu(hidden, approximate=False))
        residual = residual + low_back(highest_dot(hidden, feedforward_w[layer_index, 1].T))
    final_rows = low(layer_norm(residual, norms_w[3 * LAYERS, 0], norms_w[3 * LAYERS, 1]))
    ahead_rows = low_back(low(highest_dot(final_rows, ahead_w)))
    frames = jnp.arange(LEN, dtype=jnp.int32)
    loss_sum = jnp.zeros((), jnp.float32)
    for target_shift, objective_weight, source_rows in ((1, 1.0, final_rows), (2, ahead_weight, ahead_rows)):
        padding = jnp.zeros((CODEBOOKS, target_shift), jnp.int32)
        targets = jnp.concatenate([codes_clip[:, target_shift:], padding], axis=1)
        live_mask = jnp.concatenate([masks_clip[:, target_shift:], padding], axis=1)
        live_mask = live_mask * (frames + target_shift < length_clip).astype(jnp.int32)
        for codebook in range(CODEBOOKS):
            logits = low_back(highest_dot(source_rows, tables_w[1, codebook].T))
            row_max = lax.optimization_barrier(jnp.max(logits, axis=1))
            log_total = row_max + jnp.log(lax.optimization_barrier(jnp.sum(jnp.exp(logits - row_max[:, None]), axis=1)))
            picked = jnp.take_along_axis(logits, targets[codebook][:, None], axis=1)[:, 0]
            loss_sum = loss_sum + objective_weight * jnp.sum(live_mask[codebook].astype(jnp.float32) * (log_total - picked))
    return loss_sum / (CODEBOOKS * LEN * CLIPS)

def adamw_update(master, mean, square, gradient, factor, first_fix, second_fix, decay):
    gradient = gradient * factor
    mean_new = first_decay * mean + (1.0 - first_decay) * gradient
    square_new = second_decay * square + (1.0 - second_decay) * gradient * gradient
    change = learn_rate * (mean_new / first_fix / (jnp.sqrt(square_new / second_fix) + adam_epsilon) + decay * master)
    master_new = master - change
    return (master_new, mean_new, square_new, master_new.astype(jnp.bfloat16))

def reference(audio_codes, delay_masks, clip_lengths, text_states, step_count, attention_master, attention_mean, attention_square, feedforward_master, feedforward_mean, feedforward_square, tables_master, tables_mean, tables_square, ahead_master, ahead_mean, ahead_square, norms_master, norms_mean, norms_square):
    masters = (attention_master, feedforward_master, tables_master, ahead_master, norms_master)
    weights = tuple((master.astype(jnp.bfloat16).astype(jnp.float32) for master in masters))
    position_table = sinusoids(0.0, LEN, D)

    def total_loss(weights):

        def one_clip(carry, inputs):
            codes_clip, masks_clip, length_clip, text_clip = inputs
            value = clip_loss(weights, codes_clip, masks_clip, length_clip, text_clip.astype(jnp.float32), position_table)
            return (carry + value, None)
        summed, unused = lax.scan(jax.checkpoint(one_clip), jnp.zeros((), jnp.float32), (audio_codes, delay_masks, clip_lengths, text_states))
        return summed
    loss_value, pullback = jax.vjp(total_loss, weights)
    gradients = pullback(jnp.ones((), jnp.float32))[0]
    squares = jnp.zeros((), jnp.float32)
    for gradient in gradients:
        squares = squares + jnp.sum(gradient * gradient)
    gradient_norm = jnp.sqrt(squares)
    factor = jnp.minimum(1.0, clip_limit / (gradient_norm + 1e-06))
    step_value = step_count[0].astype(jnp.float32)
    first_fix = 1.0 - jnp.power(first_decay, step_value)
    second_fix = 1.0 - jnp.power(second_decay, step_value)
    attention_new = adamw_update(attention_master, attention_mean, attention_square, gradients[0], factor, first_fix, second_fix, weight_decay)
    feedforward_new = adamw_update(feedforward_master, feedforward_mean, feedforward_square, gradients[1], factor, first_fix, second_fix, weight_decay)
    tables_new = adamw_update(tables_master, tables_mean, tables_square, gradients[2], factor, first_fix, second_fix, weight_decay)
    ahead_new = adamw_update(ahead_master, ahead_mean, ahead_square, gradients[3], factor, first_fix, second_fix, weight_decay)
    norms_new = adamw_update(norms_master, norms_mean, norms_square, gradients[4], factor, first_fix, second_fix, 0.0)
    return (loss_value, gradient_norm, attention_new[0], attention_new[1], attention_new[2], attention_new[3], feedforward_new[0], feedforward_new[1], feedforward_new[2], feedforward_new[3], tables_new[0], tables_new[1], tables_new[2], tables_new[3], ahead_new[0], ahead_new[1], ahead_new[2], ahead_new[3], norms_new[0], norms_new[1], norms_new[2], norms_new[3])
```

```python
from functools import partial
import math

import jax
import jax.numpy as jnp
from jax import lax
from jax.experimental import pallas as pl
from jax.experimental.pallas import tpu as pltpu
from jax.sharding import PartitionSpec as P

D = 1024
HD = 64
CODEBOOKS = 4
LAYERS = 1


norm_epsilon = 1e-05
first_decay = 0.9
second_decay = 0.95
learn_rate = 0.03
weight_decay = 0.1
adam_epsilon = 1e-08
clip_limit = 0.05
ahead_weight = 0.3
masked_score = -1e30


def float_dot(left, right):
    return jnp.dot(left, right, preferred_element_type=jnp.float32)


def dot_first(left, right):
    return lax.dot_general(
        left, right, (((0,), (0,)), ((), ())), preferred_element_type=jnp.float32
    )


def dot_last(left, right):
    return lax.dot_general(
        left, right, (((1,), (1,)), ((), ())), preferred_element_type=jnp.float32
    )


def flip_bit(x, axis, bit):
    return lax.ppermute(x, axis, [(i, i ^ bit) for i in range(lax.axis_size(axis))])


def own_bit(axis, bit):
    return (lax.axis_index(axis) // bit) % 2


def bits_of(axis):
    return [1 << k for k in range(lax.axis_size(axis).bit_length() - 1)]


def device_dims():
    return [("seq", bit) for bit in reversed(bits_of("seq"))] + [
        ("fsdp", bit) for bit in reversed(bits_of("fsdp"))
    ]


def take_bit(x, position, value):
    return lax.dynamic_index_in_dim(x, value, position, keepdims=False)


def gathered(shard):
    dims = device_dims()
    order = [("fsdp", bit) for bit in reversed(bits_of("fsdp")[1:])]
    order += [("seq", bit) for bit in bits_of("seq")] + [("fsdp", 1)]
    done = []
    state = shard
    for pair in order:
        came = flip_bit(state, *pair)
        mine = own_bit(*pair) == 0
        done = [d for d in dims if d in done or d == pair]
        state = jnp.stack(
            [jnp.where(mine, state, came), jnp.where(mine, came, state)], axis=1 + done.index(pair)
        )
    return state.reshape(shard.shape[0], -1, shard.shape[2])


def halving(state, dims, order, lead):
    dims = list(dims)
    for axis, bit in order:
        position = lead + dims.index((axis, bit))
        mine = own_bit(axis, bit)
        sent = take_bit(state, position, 1 - mine).astype(jnp.bfloat16)
        came = flip_bit(sent, axis, bit)
        state = take_bit(state, position, mine) + came.astype(jnp.float32)
        dims.remove((axis, bit))
    return state


def scattered_products(pairs, row_first):
    dims = device_dims()
    seq_order = bits_of("seq") if row_first else bits_of("seq")[::-1]
    order = [("fsdp", 1)] + [("seq", bit) for bit in seq_order]
    order += [("fsdp", bit) for bit in bits_of("fsdp")[1:]]
    first, second = dims.index(order[0]), dims.index(order[1])
    rest = [k for k in range(len(dims)) if k not in (first, second)]
    rows = pairs[0][0].shape[2]
    share = rows >> len(dims)
    half, quarter = rows // 2, rows // 4
    splits = []
    for left, right in pairs:
        split = left.reshape(left.shape[:2] + (2,) * len(dims) + (share,))
        split = split.transpose(
            (2 + first, 0, 1, 2 + second) + tuple(2 + k for k in rest) + (2 + len(dims),)
        )
        splits.append(split.reshape((2,) + left.shape[:2] + (half,)))
    mine, later = own_bit(*order[0]), own_bit(*order[1])

    def products(which, start, size):
        parts = []
        for split, (left, right) in zip(splits, pairs):
            part = lax.dynamic_slice_in_dim(take_bit(split, 0, which), start, size, 2)
            parts.append(
                lax.dot_general(
                    part, right, (((1,), (1,)), ((0,), (0,))), preferred_element_type=jnp.float32
                )
            )
        return parts

    def joined(parts):
        return parts[0] if len(parts) == 1 else jnp.concatenate(parts, axis=0)

    sent = joined([part.astype(jnp.bfloat16) for part in products(1 - mine, 0, half)])
    came = flip_bit(sent, *order[0])

    def added(start):
        there = lax.dynamic_slice_in_dim(came, start, quarter, 1).astype(jnp.float32)
        parts, at = [], 0
        for part in products(mine, start, quarter):
            parts.append(part + there[at : at + part.shape[0]])
            at += part.shape[0]
        return parts

    onward = joined([part.astype(jnp.bfloat16) for part in added((1 - later) * quarter)])
    arrived = flip_bit(onward, *order[1])
    state = joined(added(later * quarter)) + arrived.astype(jnp.float32)
    state = state.reshape((state.shape[0],) + (2,) * len(rest) + (share, state.shape[2]))
    return halving(state, [dims[k] for k in rest], order[2:], 1)


def scattered_tables(full):
    dims = [("fsdp", bit) for bit in reversed(bits_of("fsdp"))]
    count, rows, width = full.shape
    state = full.reshape((count,) + (2,) * len(dims) + (rows >> len(dims), width))
    return halving(state, dims, dims[::-1], 1)


def summed_everywhere(x):
    for axis, bit in device_dims():
        x = x + flip_bit(x, axis, bit)
    return x


def by_partner(x):
    bits = bits_of("seq")
    shape = x.shape
    x = x.reshape(shape[:-1] + (2,) * len(bits) + (-1,))
    for k, bit in enumerate(reversed(bits)):
        axis = len(shape) - 1 + k
        x = jnp.where(own_bit("seq", bit) == 1, jnp.flip(x, axis), x)
    return x.reshape(shape)


def column_orders(width):
    bits = bits_of("seq")
    return [(0, width // 2, bits), (width // 2, width, bits[::-1])]


def partner_rows(rows):
    bits = bits_of("seq")[::-1]
    outs = []
    for start, stop, order in column_orders(rows.shape[1]):
        state, done = rows[:, start:stop], []
        for bit in order:
            done = [b for b in bits if b in done or b == bit]
            state = jnp.stack([state, flip_bit(state, "seq", bit)], axis=done.index(bit))
        outs.append(state.reshape(-1, stop - start))
    return jnp.concatenate(outs, axis=1)


def partner_sum(parts):
    bits = bits_of("seq")[::-1]
    outs = []
    for start, stop, order in column_orders(parts.shape[1]):
        left = list(bits)
        state = parts[:, start:stop].reshape((2,) * len(bits) + (-1, stop - start))
        for bit in order:
            axis = left.index(bit)
            sent = lax.index_in_dim(state, 1, axis, keepdims=False)
            state = lax.index_in_dim(state, 0, axis, keepdims=False) + flip_bit(sent, "seq", bit)
            left.remove(bit)
        outs.append(state)
    return jnp.concatenate(outs, axis=1)


def spread_kernel(tile_ref, all_ref, send_sem, recv_sem):
    seq_count, fsdp_count = lax.axis_size("seq"), lax.axis_size("fsdp")
    count = seq_count * fsdp_count
    me = lax.axis_index("seq") * fsdp_count + lax.axis_index("fsdp")

    def place(k):
        return {"seq": k // fsdp_count, "fsdp": lax.rem(k, fsdp_count)}

    barrier = pltpu.get_barrier_semaphore()

    def greet(k, carry):
        pl.semaphore_signal(
            barrier,
            inc=1,
            device_id=place(lax.rem(me + k, count)),
            device_id_type=pl.DeviceIdType.MESH,
        )
        return carry

    lax.fori_loop(1, count, greet, 0)
    pl.semaphore_wait(barrier, count - 1)

    def copy(k):
        return pltpu.make_async_remote_copy(
            src_ref=tile_ref,
            dst_ref=all_ref.at[me],
            send_sem=send_sem.at[k],
            recv_sem=recv_sem.at[k],
            device_id=place(lax.rem(me + k, count)),
            device_id_type=pl.DeviceIdType.MESH,
        )

    def send(k, carry):
        copy(k).start()
        return carry

    def wait(k, carry):
        copy(k).wait()
        return carry

    lax.fori_loop(1, count, send, 0)
    all_ref[me] = tile_ref[...]
    lax.fori_loop(1, count, wait, 0)


def spread(tile, collective_id):
    count = lax.axis_size("seq") * lax.axis_size("fsdp")
    return pl.pallas_call(
        spread_kernel,
        out_shape=jax.ShapeDtypeStruct((count,) + tile.shape, tile.dtype),
        in_specs=[pl.BlockSpec(memory_space=pltpu.VMEM)],
        out_specs=pl.BlockSpec(memory_space=pltpu.VMEM),
        scratch_shapes=[pltpu.SemaphoreType.DMA((count,)), pltpu.SemaphoreType.DMA((count,))],
        compiler_params=pltpu.CompilerParams(collective_id=collective_id, has_side_effects=True),
        name=f"spread_{collective_id}",
    )(tile)


def as_tile(values):
    return jnp.pad(values, (0, 1024 - values.shape[0])).reshape(8, 128)


def layer_norm(residual, gain, bias):
    centered = residual - jnp.mean(residual, axis=-1, keepdims=True)
    variance = jnp.mean(centered * centered, axis=-1, keepdims=True)
    return centered * lax.rsqrt(variance + norm_epsilon) * gain + bias


def sinusoids(offset, row_count, width):
    half_width = width // 2
    log_rate = math.log(10000.0) / (half_width - 1)
    frequency = jnp.exp(jnp.arange(half_width, dtype=jnp.float32) * -log_rate)
    places = (offset + jnp.arange(row_count, dtype=jnp.float32))[:, None] * frequency[None, :]
    return jnp.concatenate([jnp.cos(places), jnp.sin(places)], axis=1)


def to_heads(rows):
    count = lax.axis_size("seq")
    tokens, width = rows.shape
    blocks = rows.reshape(tokens, count, width // count).transpose(1, 0, 2)
    blocks = lax.all_to_all(blocks, "seq", split_axis=0, concat_axis=0, tiled=True)
    return blocks.reshape(count * tokens, width // count)


def to_rows(heads):
    count = lax.axis_size("seq")
    tokens, width = heads.shape[0] // count, heads.shape[1]
    blocks = heads.reshape(count, tokens, width)
    blocks = lax.all_to_all(blocks, "seq", split_axis=0, concat_axis=0, tiled=True)
    return blocks.transpose(1, 0, 2).reshape(tokens, count * width)


def block_size():
    return 512


def causal_forward(queries, key_rows, value_rows):
    total_rows = queries.shape[0]
    block_rows = block_size()
    scale_factor = 1.0 / math.sqrt(queries.shape[2])
    outputs = []
    totals = []
    for block_index in range(total_rows // block_rows):
        start_row = block_index * block_rows
        stop_row = start_row + block_rows
        scores = (
            jnp.einsum(
                "qhd,khd->hqk",
                queries[start_row:stop_row],
                key_rows[:stop_row],
                preferred_element_type=jnp.float32,
            )
            * scale_factor
        )
        allowed = (start_row + jnp.arange(block_rows))[:, None] >= jnp.arange(stop_row)[None, :]
        scores = jnp.where(allowed[None], scores, masked_score)
        row_max = jnp.max(scores, axis=2, keepdims=True)
        exponent = jnp.exp(scores - row_max)
        row_sum = jnp.sum(exponent, axis=2, keepdims=True)
        probs_low = (exponent / row_sum).astype(jnp.bfloat16)
        outputs.append(
            jnp.einsum(
                "hqk,khd->qhd", probs_low, value_rows[:stop_row], preferred_element_type=jnp.float32
            )
        )
        totals.append(row_max + jnp.log(row_sum))
    return (jnp.concatenate(outputs, axis=0), jnp.concatenate(totals, axis=1))


def causal_backward(queries, key_rows, value_rows, log_totals, grad_out):
    total_rows = queries.shape[0]
    block_rows = block_size()
    scale_factor = 1.0 / math.sqrt(queries.shape[2])
    grad_queries = []
    grad_keys = jnp.zeros(key_rows.shape, jnp.float32)
    grad_values = jnp.zeros(value_rows.shape, jnp.float32)
    for block_index in range(total_rows // block_rows):
        start_row = block_index * block_rows
        stop_row = start_row + block_rows
        query_part = queries[start_row:stop_row]
        out_part = grad_out[start_row:stop_row]
        scores = (
            jnp.einsum(
                "qhd,khd->hqk", query_part, key_rows[:stop_row], preferred_element_type=jnp.float32
            )
            * scale_factor
        )
        allowed = (start_row + jnp.arange(block_rows))[:, None] >= jnp.arange(stop_row)[None, :]
        scores = jnp.where(allowed[None], scores, masked_score)
        attention_probs = jnp.exp(scores - log_totals[:, start_row:stop_row])
        probs_low = attention_probs.astype(jnp.bfloat16)
        grad_probs = jnp.einsum(
            "qhd,khd->hqk", out_part, value_rows[:stop_row], preferred_element_type=jnp.float32
        )
        grad_scores = attention_probs * (
            grad_probs - jnp.sum(attention_probs * grad_probs, axis=2, keepdims=True)
        )
        scores_low = grad_scores.astype(jnp.bfloat16)
        grad_queries.append(
            scale_factor
            * jnp.einsum(
                "hqk,khd->qhd", scores_low, key_rows[:stop_row], preferred_element_type=jnp.float32
            )
        )
        grad_keys = grad_keys.at[:stop_row].add(
            scale_factor
            * jnp.einsum("hqk,qhd->khd", scores_low, query_part, preferred_element_type=jnp.float32)
        )
        grad_values = grad_values.at[:stop_row].add(
            jnp.einsum("hqk,qhd->khd", probs_low, out_part, preferred_element_type=jnp.float32)
        )
    return (jnp.concatenate(grad_queries, axis=0), grad_keys, grad_values)


def cross_forward(queries, key_rows, value_rows):
    scale_factor = 1.0 / math.sqrt(queries.shape[2])
    scores = (
        jnp.einsum("qhd,khd->hqk", queries, key_rows, preferred_element_type=jnp.float32)
        * scale_factor
    )
    row_max = jnp.max(scores, axis=2, keepdims=True)
    exponent = jnp.exp(scores - row_max)
    row_sum = jnp.sum(exponent, axis=2, keepdims=True)
    probs_low = (exponent / row_sum).astype(jnp.bfloat16)
    output = jnp.einsum("hqk,khd->qhd", probs_low, value_rows, preferred_element_type=jnp.float32)
    return (output, row_max + jnp.log(row_sum))


def cross_backward(queries, key_rows, value_rows, log_totals, grad_out):
    scale_factor = 1.0 / math.sqrt(queries.shape[2])
    scores = (
        jnp.einsum("qhd,khd->hqk", queries, key_rows, preferred_element_type=jnp.float32)
        * scale_factor
    )
    attention_probs = jnp.exp(scores - log_totals)
    probs_low = attention_probs.astype(jnp.bfloat16)
    grad_probs = jnp.einsum(
        "qhd,khd->hqk", grad_out, value_rows, preferred_element_type=jnp.float32
    )
    grad_scores = attention_probs * (
        grad_probs - jnp.sum(attention_probs * grad_probs, axis=2, keepdims=True)
    )
    scores_low = grad_scores.astype(jnp.bfloat16)
    grad_queries = scale_factor * jnp.einsum(
        "hqk,khd->qhd", scores_low, key_rows, preferred_element_type=jnp.float32
    )
    grad_keys = scale_factor * jnp.einsum(
        "hqk,qhd->khd", scores_low, queries, preferred_element_type=jnp.float32
    )
    grad_values = jnp.einsum(
        "hqk,qhd->khd", probs_low, grad_out, preferred_element_type=jnp.float32
    )
    return (grad_queries, grad_keys, grad_values)


def layer_forward(residual, gathered, text_clip, seq_index, seq_count):
    matrices, feedforward_w, norm_params = gathered
    norm_float = norm_params.astype(jnp.float32)
    head_width = matrices[0].shape[1] // seq_count
    heads_here = head_width // HD
    text_rows = text_clip.shape[0]
    normed_self = layer_norm(residual, norm_float[0, 0], norm_float[0, 1]).astype(jnp.bfloat16)
    queries, key_rows, value_rows = (
        to_heads(float_dot(normed_self, matrices[k]).astype(jnp.bfloat16)).reshape(
            -1, heads_here, HD
        )
        for k in range(3)
    )
    total_rows = queries.shape[0]
    attended, self_totals = causal_forward(queries, key_rows, value_rows)
    self_rows = to_rows(attended.astype(jnp.bfloat16).reshape(total_rows, head_width))
    after_self = residual + float_dot(self_rows, matrices[3])
    normed_cross = layer_norm(after_self, norm_float[1, 0], norm_float[1, 1]).astype(jnp.bfloat16)
    cross_query = float_dot(normed_cross, matrices[4]).astype(jnp.bfloat16)
    cross_heads = to_heads(cross_query).reshape(total_rows, heads_here, HD)
    column_start = seq_index * head_width
    key_columns = lax.dynamic_slice_in_dim(matrices[5], column_start, head_width, 1)
    value_columns = lax.dynamic_slice_in_dim(matrices[6], column_start, head_width, 1)
    cross_keys = (
        float_dot(text_clip, key_columns).astype(jnp.bfloat16).reshape(text_rows, heads_here, HD)
    )
    cross_values = (
        float_dot(text_clip, value_columns).astype(jnp.bfloat16).reshape(text_rows, heads_here, HD)
    )
    cross_out, cross_totals = cross_forward(cross_heads, cross_keys, cross_values)
    cross_rows = to_rows(cross_out.astype(jnp.bfloat16).reshape(total_rows, head_width))
    after_cross = after_self + float_dot(cross_rows, matrices[7])
    normed_feed = layer_norm(after_cross, norm_float[2, 0], norm_float[2, 1]).astype(jnp.bfloat16)
    hidden_pre = float_dot(normed_feed, feedforward_w[0])
    hidden_low = jax.nn.gelu(hidden_pre, approximate=False).astype(jnp.bfloat16)
    output = after_cross + dot_last(hidden_low, feedforward_w[1])
    saved = (
        normed_self,
        queries,
        key_rows,
        value_rows,
        self_totals,
        self_rows,
        after_self,
        normed_cross,
        cross_heads,
        cross_keys,
        cross_values,
        cross_totals,
        cross_rows,
        after_cross,
        normed_feed,
        hidden_pre,
        hidden_low,
    )
    return (output, saved)


def layer_backward(
    residual, gathered, text_clip, saved, grad_residual, seq_index, seq_count, ahead_left, ahead_right
):
    matrices, feedforward_w, norm_params = gathered
    norm_float = norm_params.astype(jnp.float32)
    (
        normed_self,
        queries,
        key_rows,
        value_rows,
        self_totals,
        self_rows,
        after_self,
        normed_cross,
        cross_heads,
        cross_keys,
        cross_values,
        cross_totals,
        cross_rows,
        after_cross,
        normed_feed,
        hidden_pre,
        hidden_low,
    ) = saved
    head_width = matrices[0].shape[1] // seq_count
    heads_here = head_width // HD
    total_rows = queries.shape[0]
    text_rows = text_clip.shape[0]
    column_start = seq_index * head_width
    branch_low = grad_residual.astype(jnp.bfloat16)
    down_left = branch_low
    grad_hidden = float_dot(branch_low, feedforward_w[1])
    unused_gelu, gelu_pull = jax.vjp(partial(jax.nn.gelu, approximate=False), hidden_pre)
    grad_pre = gelu_pull(grad_hidden)[0].astype(jnp.bfloat16)
    feed_grads = scattered_products(
        [(normed_feed[None], grad_pre[None]), (down_left[None], hidden_low[None])], True
    )
    grad_normed = dot_last(grad_pre, feedforward_w[0])
    unused_norm, norm_pull = jax.vjp(layer_norm, after_cross, norm_float[2, 0], norm_float[2, 1])
    grad_inner, feed_gain, feed_bias = norm_pull(grad_normed)
    grad_residual = grad_residual + grad_inner
    branch_low = grad_residual.astype(jnp.bfloat16)
    cross_branch = branch_low
    grad_rows = dot_last(branch_low, matrices[7]).astype(jnp.bfloat16)
    grad_heads = to_heads(grad_rows).reshape(total_rows, heads_here, HD)
    grad_cq, grad_ck, grad_cv = cross_backward(
        cross_heads, cross_keys, cross_values, cross_totals, grad_heads
    )
    grad_cq_rows = to_rows(grad_cq.astype(jnp.bfloat16).reshape(total_rows, head_width))
    grad_normed = dot_last(grad_cq_rows, matrices[4])
    key_low = grad_ck.reshape(text_rows, head_width).astype(jnp.bfloat16)
    value_low = grad_cv.reshape(text_rows, head_width).astype(jnp.bfloat16)
    wide = jnp.zeros((text_rows, head_width * seq_count), jnp.bfloat16)
    wide_key = lax.dynamic_update_slice(wide, key_low, (0, column_start))
    wide_value = lax.dynamic_update_slice(wide, value_low, (0, column_start))
    unused_norm, norm_pull = jax.vjp(layer_norm, after_self, norm_float[1, 0], norm_float[1, 1])
    grad_inner, cross_gain, cross_bias = norm_pull(grad_normed)
    grad_residual = grad_residual + grad_inner
    branch_low = grad_residual.astype(jnp.bfloat16)
    early_grads = scattered_products(
        [
            (self_rows[None], branch_low[None]),
            (normed_cross[None], grad_cq_rows[None]),
            (jnp.stack([text_clip, text_clip]), jnp.stack([wide_key, wide_value])),
            (cross_rows[None], cross_branch[None]),
            (ahead_left[None], ahead_right[None]),
        ],
        False,
    )
    grad_rows = dot_last(branch_low, matrices[3]).astype(jnp.bfloat16)
    grad_heads = to_heads(grad_rows).reshape(total_rows, heads_here, HD)
    grad_q, grad_k, grad_v = causal_backward(queries, key_rows, value_rows, self_totals, grad_heads)
    grad_parts = [
        to_rows(part.astype(jnp.bfloat16).reshape(total_rows, head_width))
        for part in (grad_q, grad_k, grad_v)
    ]
    late_grads = scattered_products([(normed_self[None], part[None]) for part in grad_parts], True)
    grad_normed = (
        dot_last(grad_parts[0], matrices[0])
        + dot_last(grad_parts[1], matrices[1])
        + dot_last(grad_parts[2], matrices[2])
    )
    unused_norm, norm_pull = jax.vjp(layer_norm, residual, norm_float[0, 0], norm_float[0, 1])
    grad_inner, self_gain, self_bias = norm_pull(grad_normed)
    grad_residual = grad_residual + grad_inner
    grad_norms = jnp.stack(
        [
            jnp.stack([self_gain, self_bias]),
            jnp.stack([cross_gain, cross_bias]),
            jnp.stack([feed_gain, feed_bias]),
        ],
        axis=0,
    )
    return (grad_residual, late_grads, early_grads, feed_grads, grad_norms)


def adamw_update(master, mean, square, gradient, factor, first_fix, second_fix, decay):
    gradient = gradient * factor
    mean_new = first_decay * mean + (1.0 - first_decay) * gradient
    square_new = second_decay * square + (1.0 - second_decay) * gradient * gradient
    change = learn_rate * (
        mean_new / first_fix / (jnp.sqrt(square_new / second_fix) + adam_epsilon) + decay * master
    )
    master_new = master - change
    return (master_new, mean_new, square_new, master_new.astype(jnp.bfloat16))


def on_device(
    audio_codes,
    delay_masks,
    clip_lengths,
    text_states,
    step_count,
    attention_master,
    attention_mean,
    attention_square,
    feedforward_master,
    feedforward_mean,
    feedforward_square,
    tables_master,
    tables_mean,
    tables_square,
    ahead_master,
    ahead_mean,
    ahead_square,
    norms_master,
    norms_mean,
    norms_square,
):
    seq_count = lax.axis_size("seq")
    seq_index = lax.axis_index("seq")
    clips_total = lax.axis_size("fsdp")
    codes_clip = audio_codes[0]
    masks_clip = delay_masks[0]
    length_clip = clip_lengths[0]
    text_clip = text_states[0]
    total_rows = codes_clip.shape[1]
    rows_here = total_rows // seq_count
    row_start = seq_index * rows_here
    scale_norm = 1.0 / (CODEBOOKS * total_rows * clips_total)
    attention_low = attention_master.astype(jnp.bfloat16)
    feedforward_low = feedforward_master.astype(jnp.bfloat16)
    tables_low = tables_master.astype(jnp.bfloat16)
    ahead_low = ahead_master.astype(jnp.bfloat16)
    norms_low = norms_master.astype(jnp.bfloat16)
    share = norms_low.shape[2]
    norms_all = (
        spread(as_tile(norms_low.astype(jnp.float32).reshape(-1)), 0)
        .reshape(-1, 1024)[:, : norms_low.size]
        .reshape((-1,) + norms_low.shape)
        .transpose(1, 2, 0, 3)
        .reshape(norms_low.shape[0], 2, D)
    )
    qkv_all = gathered(attention_low[0, :3])
    embed_part = lax.all_gather(tables_low[0], "fsdp", axis=1, tiled=True)
    vocab_part = embed_part.shape[1]
    vocab_start = seq_index * vocab_part
    vocab_range = jnp.arange(vocab_part, dtype=jnp.int32)
    local_ids = by_partner(codes_clip) - vocab_start
    onehot_ids = (
        (local_ids.T[:, :, None] == vocab_range[None, None, :])
        .astype(jnp.bfloat16)
        .reshape(total_rows, CODEBOOKS * vocab_part)
    )
    embed_sum = float_dot(onehot_ids, embed_part.reshape(CODEBOOKS * vocab_part, D))
    residual = partner_sum(embed_sum) + sinusoids(row_start.astype(jnp.float32), rows_here, D)
    both = ("seq", "fsdp")
    matrices = [qkv_all[k] for k in range(3)] + [
        lax.all_gather(attention_low[0, k], both, axis=0, tiled=True) for k in range(3, 8)
    ]
    feed_all = [lax.all_gather(feedforward_low[0, k], both, axis=0, tiled=True) for k in range(2)]
    ahead_full = lax.all_gather(ahead_low, both, axis=0, tiled=True)
    heads_part = lax.all_gather(tables_low[1], "fsdp", axis=1, tiled=True)
    heads_rows = heads_part.reshape(CODEBOOKS * vocab_part, D)
    gathered_layer = (matrices, feed_all, norms_all[:3])
    final_float = norms_all[3 * LAYERS]
    layer_input = residual
    residual, saved = layer_forward(residual, gathered_layer, text_clip, seq_index, seq_count)
    final_low = layer_norm(residual, final_float[0], final_float[1]).astype(jnp.bfloat16)
    final_all = partner_rows(final_low)
    ahead_all = float_dot(final_all, ahead_full).astype(jnp.bfloat16)
    frames = jnp.arange(total_rows, dtype=jnp.int32)
    target_sets = []
    for target_shift in (1, 2):
        padding = jnp.zeros((CODEBOOKS, target_shift), jnp.int32)
        targets = jnp.concatenate([codes_clip[:, target_shift:], padding], axis=1)
        live_mask = jnp.concatenate([masks_clip[:, target_shift:], padding], axis=1)
        live_mask = live_mask * (frames + target_shift < length_clip).astype(jnp.int32)
        target_sets.append(
            (by_partner(targets) - vocab_start, by_partner(live_mask).astype(jnp.float32))
        )
    sources = (final_all, ahead_all)
    logit_blocks = []
    stats = []
    for objective_index in range(2):
        local_targets, live_mask = target_sets[objective_index]
        for codebook in range(CODEBOOKS):
            logits = dot_last(sources[objective_index], heads_part[codebook])
            row_max = jnp.max(logits, axis=1)
            row_sum = jnp.sum(jnp.exp(logits - row_max[:, None]), axis=1)
            hit = vocab_range[None, :] == local_targets[codebook][:, None]
            picked = jnp.sum(jnp.where(hit, logits, 0.0), axis=1)
            logit_blocks.append(logits)
            stats.append(jnp.stack([row_max, row_sum, picked]))
    own_stats = by_partner(jnp.stack(stats, axis=1))
    all_stats = lax.all_gather(own_stats.reshape(-1, total_rows), "seq")
    all_stats = by_partner(all_stats.reshape((seq_count,) + own_stats.shape))
    merged_max = jnp.max(all_stats[:, 0], axis=0)
    merged_sum = jnp.sum(all_stats[:, 1] * jnp.exp(all_stats[:, 0] - merged_max), axis=0)
    merged_pick = jnp.sum(all_stats[:, 2], axis=0)
    log_totals = merged_max + jnp.log(merged_sum)
    factors = jnp.array([1.0] * CODEBOOKS + [ahead_weight] * CODEBOOKS, jnp.float32)[:, None]
    weighted = factors * jnp.concatenate([target_sets[0][1], target_sets[1][1]], axis=0)
    own_loss = jnp.sum((weighted * (log_totals - merged_pick))[:, :rows_here])
    grad_parts = []
    head_grads = None
    for objective_index in range(2):
        local_targets, live_mask = target_sets[objective_index]
        lows = []
        for codebook in range(CODEBOOKS):
            position = objective_index * CODEBOOKS + codebook
            probs = jnp.exp(logit_blocks[position] - log_totals[position][:, None])
            onehot = (vocab_range[None, :] == local_targets[codebook][:, None]).astype(jnp.float32)
            coefficient = (weighted[position] * scale_norm)[:, None]
            lows.append((coefficient * (probs - onehot)).astype(jnp.bfloat16))
        grad_low = jnp.concatenate(lows, axis=1)
        grad_parts.append(float_dot(grad_low, heads_rows))
        product = dot_first(grad_low, sources[objective_index])
        head_grads = product if head_grads is None else head_grads + product
    heads_shard = scattered_tables(head_grads.reshape(CODEBOOKS, vocab_part, D))
    ahead_grad_low = grad_parts[1].astype(jnp.bfloat16)
    grad_final = partner_sum(grad_parts[0] + dot_last(ahead_grad_low, ahead_full))
    unused_norm, final_pull = jax.vjp(layer_norm, residual, final_float[0], final_float[1])
    grad_residual, final_gain, final_bias = final_pull(grad_final)
    grad_residual, late_grads, early_grads, feedforward_grad, norm_grads = layer_backward(
        layer_input,
        gathered_layer,
        text_clip,
        saved,
        grad_residual,
        seq_index,
        seq_count,
        final_all,
        ahead_grad_low,
    )
    embed_grad_all = partner_rows(grad_residual.astype(jnp.bfloat16))
    embed_grads = dot_first(onehot_ids, embed_grad_all)
    embed_shard = scattered_tables(embed_grads.reshape(CODEBOOKS, vocab_part, D))
    tables_grad_shard = jnp.stack([embed_shard, heads_shard])
    attention_grad = jnp.concatenate([late_grads, early_grads[:5]], axis=0)[None]
    feedforward_grad = feedforward_grad[None]
    ahead_grad_shard = early_grads[5]
    norms_local = jnp.concatenate([norm_grads, jnp.stack([final_gain, final_bias])[None]], axis=0)
    norms_total = summed_everywhere(norms_local.reshape(-1, D))
    place = seq_index * clips_total + lax.axis_index("fsdp")
    norms_grad = lax.dynamic_slice_in_dim(norms_total, place * share, share, 1)
    norms_grad = norms_grad.reshape(norms_master.shape)
    squares = (
        jnp.sum(attention_grad * attention_grad)
        + jnp.sum(feedforward_grad * feedforward_grad)
        + jnp.sum(tables_grad_shard * tables_grad_shard)
        + jnp.sum(ahead_grad_shard * ahead_grad_shard)
        + jnp.sum(norms_grad * norms_grad)
    )
    totals = jnp.sum(spread(as_tile(jnp.stack([squares, own_loss])), 1)[:, 0, :2], axis=0)
    total_squares, total_loss = totals[0], totals[1]
    gradient_norm = jnp.sqrt(total_squares)
    loss_value = total_loss * scale_norm
    factor = jnp.minimum(1.0, clip_limit / (gradient_norm + 1e-06))
    step_value = step_count[0].astype(jnp.float32)
    first_fix = 1.0 - jnp.power(first_decay, step_value)
    second_fix = 1.0 - jnp.power(second_decay, step_value)
    attention_new = adamw_update(
        attention_master,
        attention_mean,
        attention_square,
        attention_grad,
        factor,
        first_fix,
        second_fix,
        weight_decay,
    )
    feedforward_new = adamw_update(
        feedforward_master,
        feedforward_mean,
        feedforward_square,
        feedforward_grad,
        factor,
        first_fix,
        second_fix,
        weight_decay,
    )
    tables_new = adamw_update(
        tables_master,
        tables_mean,
        tables_square,
        tables_grad_shard,
        factor,
        first_fix,
        second_fix,
        weight_decay,
    )
    ahead_new = adamw_update(
        ahead_master,
        ahead_mean,
        ahead_square,
        ahead_grad_shard,
        factor,
        first_fix,
        second_fix,
        weight_decay,
    )
    norms_new = adamw_update(
        norms_master, norms_mean, norms_square, norms_grad, factor, first_fix, second_fix, 0.0
    )
    return (
        loss_value,
        gradient_norm,
        attention_new[0],
        attention_new[1],
        attention_new[2],
        attention_new[3],
        feedforward_new[0],
        feedforward_new[1],
        feedforward_new[2],
        feedforward_new[3],
        tables_new[0],
        tables_new[1],
        tables_new[2],
        tables_new[3],
        ahead_new[0],
        ahead_new[1],
        ahead_new[2],
        ahead_new[3],
        norms_new[0],
        norms_new[1],
        norms_new[2],
        norms_new[3],
    )


def solution(mesh):
    placed = (
        P("fsdp", None, None),
        P("fsdp", None, None),
        P("fsdp"),
        P("fsdp", None, None),
        P(),
        P(None, None, ("seq", "fsdp"), None),
        P(None, None, ("seq", "fsdp"), None),
        P(None, None, ("seq", "fsdp"), None),
        P(None, None, ("seq", "fsdp"), None),
        P(None, None, ("seq", "fsdp"), None),
        P(None, None, ("seq", "fsdp"), None),
        P(None, None, ("seq", "fsdp"), None),
        P(None, None, ("seq", "fsdp"), None),
        P(None, None, ("seq", "fsdp"), None),
        P(("seq", "fsdp"), None),
        P(("seq", "fsdp"), None),
        P(("seq", "fsdp"), None),
        P(None, None, ("seq", "fsdp")),
        P(None, None, ("seq", "fsdp")),
        P(None, None, ("seq", "fsdp")),
    )
    return jax.shard_map(
        on_device,
        mesh=mesh,
        in_specs=placed,
        out_specs=(
            P(),
            P(),
            P(None, None, ("seq", "fsdp"), None),
            P(None, None, ("seq", "fsdp"), None),
            P(None, None, ("seq", "fsdp"), None),
            P(None, None, ("seq", "fsdp"), None),
            P(None, None, ("seq", "fsdp"), None),
            P(None, None, ("seq", "fsdp"), None),
            P(None, None, ("seq", "fsdp"), None),
            P(None, None, ("seq", "fsdp"), None),
            P(None, None, ("seq", "fsdp"), None),
            P(None, None, ("seq", "fsdp"), None),
            P(None, None, ("seq", "fsdp"), None),
            P(None, None, ("seq", "fsdp"), None),
            P(("seq", "fsdp"), None),
            P(("seq", "fsdp"), None),
            P(("seq", "fsdp"), None),
            P(("seq", "fsdp"), None),
            P(None, None, ("seq", "fsdp")),
            P(None, None, ("seq", "fsdp")),
            P(None, None, ("seq", "fsdp")),
            P(None, None, ("seq", "fsdp")),
        ),
        check_vma=False,
    )
```
